32 devices in a mesh: lib: 2 (over y), row: 4 (over z), col: 4 (over x, core).
Axes of the slice: x: 2, y: 2, z: 4, core: 2. Of those that a mesh axis runs over, the one named last changes fastest.
Arguments:
- abundance: float32 [1024, 128, 1024], P('lib', 'row', 'col'), may hold values from 0 to 1
- duals: float32 [2, 1024, 128, 1024], P(None, 'lib', 'row', 'col'), may hold values from -1 to 1
- reflectance: bfloat16 [224, 128, 1024], P(None, 'row', 'col'), may hold values from -6 to 6
- library: bfloat16 [224, 1024], P(None, 'lib'), may hold values from -0.375 to 0.375
Outputs:
- abund_next: float32 [1024, 128, 1024], P('lib', 'row', 'col')
- duals_next: float32 [2, 1024, 128, 1024], P(None, 'lib', 'row', 'col')
The draws below stay inside these ranges and needn't reach their ends.
All inputs are finite; a program needn't handle non-finite values.
Results may differ from the reference program's by a relative error of at most 0.0018.
Values may be sent and summed in bfloat16 or wider, within the bound.
A program may use at most 384 MiB of HBM per device.

```python
import jax
import jax.numpy as jnp
from jax import lax

B = 224
M = 1024
PASSES = 3
NH = 128
NW = 1024


def steps_of(rng, extent, cuts, least, largest):
    factor_of = 1.0
    for axis_at, parts in cuts:
        draws = jax.random.uniform(jax.random.fold_in(jax.random.fold_in(rng, 6), axis_at), (parts,), jnp.float32, least / len(cuts), largest / len(cuts))
        factor_of = factor_of * jnp.repeat(jnp.exp(draws), extent[axis_at] // parts).reshape((-1,) + (1,) * (len(extent) - 1 - axis_at))
    return factor_of


def centred(rng, dims, spread, most, pieces=(), held_as=jnp.bfloat16):
    gain = steps_of(rng, dims, pieces, -0.22, 0.18) if pieces else 1.0
    result = jax.random.normal(rng, dims, jnp.float32) * spread * gain
    return jnp.minimum(jnp.maximum(result, -most), most).astype(held_as)


def setup_inputs(seed: int = 0) -> dict:
    keys = jax.random.split(jax.random.key(seed), 5)
    return {
        "abundance": jnp.clip(1.0 * jax.random.uniform(keys[0], (M, NH, NW), jnp.float32) ** steps_of(keys[0], (M, NH, NW), ((0, 2), (1, 4), (2, 4)), -0.2, 0.2), 0.0, 1.0),
        "duals": jnp.clip(jax.random.uniform(keys[1], (2, M, NH, NW), jnp.float32, -1.0, 1.0) * steps_of(keys[1], (2, M, NH, NW), ((1, 2), (2, 4), (3, 4)), -0.4, 0.0), -1.0, 1.0),
        "reflectance": centred(keys[2], (B, NH, NW), 1.0, 6.0, ((1, 4), (2, 4))),
        "library": centred(keys[3], (B, M), B ** -0.5, 0.375, ((1, 2),)),
    }


def divergence(dual):
    first = dual[0]
    second = dual[1]
    down = first - jnp.pad(first, ((0, 0), (1, 0), (0, 0)))[:, :-1, :]
    right = second - jnp.pad(second, ((0, 0), (0, 0), (1, 0)))[:, :, :-1]
    return down + right


def gradient(field):
    down = jnp.pad(field[:, 1:, :] - field[:, :-1, :], ((0, 0), (0, 1), (0, 0)))
    right = jnp.pad(field[:, :, 1:] - field[:, :, :-1], ((0, 0), (0, 0), (0, 1)))
    return jnp.stack([down, right])


def reference(abundance, duals, reflectance, library):
    flat = abundance.astype(jnp.bfloat16).reshape(M, NH * NW)
    resid = jnp.dot(library, flat, preferred_element_type=jnp.float32) - reflectance.reshape(B, NH * NW).astype(jnp.float32)
    descent = jnp.dot(library.T, resid.astype(jnp.bfloat16), preferred_element_type=jnp.float32)
    descent = descent.reshape(M, NH, NW).astype(abundance.dtype)
    keep_rows = (jnp.arange(NH) < NH - 1).astype(abundance.dtype)[:, None]
    keep_cols = (jnp.arange(NW) < NW - 1).astype(abundance.dtype)[None, :]
    group = min(M, 128)
    blocks = M // group

    def solve(items):
        current, direction, dual = items
        start = current - 0.1 * direction
        dual = jnp.stack([dual[0] * keep_rows, dual[1] * keep_cols])
        for step in range(PASSES):
            field = start - 0.25 * divergence(dual)
            dual = jnp.clip(dual + 0.5 * gradient(field), -1.0, 1.0)
        final = start - 0.25 * divergence(dual)
        return jnp.maximum(final - 0.02, 0.0), dual

    stacked = jnp.swapaxes(duals.reshape(2, blocks, group, NH, NW), 0, 1)
    abund_next, dual_next = lax.map(solve, (abundance.reshape(blocks, group, NH, NW), descent.reshape(blocks, group, NH, NW), stacked))
    abund_next = abund_next.reshape(M, NH, NW)
    dual_next = jnp.swapaxes(dual_next, 0, 1).reshape(2, M, NH, NW)
    return abund_next, dual_next
```

```python
import functools

import jax
import jax.numpy as jnp
from jax import lax
from jax.experimental import pallas as pl
from jax.experimental.pallas import tpu as pltpu
from jax.sharding import PartitionSpec as P

PASSES = 3
HALO = PASSES + 1
LANES = 128
BLOCK = 16


def shifted(array, axis, by):
    length = lax.axis_size(axis)
    pairs = [(i, i + by) for i in range(length) if 0 <= i + by < length]
    return lax.ppermute(array, axis, pairs)


def row_halo(array):
    height = array.shape[-2]
    below = shifted(array[..., :HALO, :], "row", -1)
    above = shifted(array[..., height - HALO :, :], "row", 1)
    return jnp.concatenate([below, above], axis=-2)


def col_halo(array, rows):
    width = array.shape[-1]

    def edge(at):
        cut = jnp.concatenate([array[..., at : at + HALO], rows[..., at : at + HALO]], axis=-2)
        return jnp.moveaxis(cut, -3, -1)

    right = shifted(edge(0), "col", -1)
    left = shifted(edge(width - HALO), "col", 1)
    gap = jnp.zeros(right.shape[:-2] + (LANES - 2 * HALO,) + right.shape[-1:], right.dtype)
    both = jnp.concatenate([right, gap, left], axis=-2)
    return jnp.moveaxis(both, -1, -3)


def step_kernel(start_ref, dual_ref, sr_ref, sc_ref, dr_ref, dc_ref, keep_ref, out_ref, dual_out_ref):
    _, height, width = start_ref.shape
    keep0 = keep_ref[0]
    keep1 = keep_ref[1]
    tall, wide = keep0.shape

    def extended(main, rows, cols):
        cols = cols.astype(jnp.float32)
        upper = jnp.concatenate([main, cols[:height]], axis=1)
        lower = jnp.concatenate([rows.astype(jnp.float32), cols[height:]], axis=1)
        return jnp.concatenate([upper, lower], axis=0)

    def one(i, carry):
        start = extended(start_ref[i], sr_ref[i], sc_ref[i])
        q0 = extended(dual_ref[0, i], dr_ref[0, i], dc_ref[0, i]) * keep0
        q1 = extended(dual_ref[1, i], dr_ref[1, i], dc_ref[1, i]) * keep1

        def field(q0, q1):
            return start - 0.25 * (q0 - pltpu.roll(q0, 1, 0) + (q1 - pltpu.roll(q1, 1, 1)))

        for _ in range(PASSES):
            z = field(q0, q1)
            half = 0.5 * z
            down = pltpu.roll(half, tall - 1, 0) - half
            right = pltpu.roll(half, wide - 1, 1) - half
            q0 = jnp.clip(q0 + down * keep0, -1.0, 1.0)
            q1 = jnp.clip(q1 + right * keep1, -1.0, 1.0)
        final = field(q0, q1)
        out_ref[i] = jnp.maximum(final[:height, :width] - 0.02, 0.0)
        dual_out_ref[0, i] = q0[:height, :width]
        dual_out_ref[1, i] = q1[:height, :width]
        return carry

    lax.fori_loop(0, start_ref.shape[0], one, 0)


def on_device(abundance, duals, reflectance, library):
    maps, height, width = abundance.shape
    total_rows = height * lax.axis_size("row")
    total_cols = width * lax.axis_size("col")
    tall, wide = height + 2 * HALO, width + LANES
    r = lax.broadcasted_iota(jnp.int32, (tall, wide), 0)
    c = lax.broadcasted_iota(jnp.int32, (tall, wide), 1)
    r = jnp.where(r >= tall - HALO, r - tall, r) + lax.axis_index("row") * height
    c = jnp.where(c >= wide - HALO, c - wide, c) + lax.axis_index("col") * width
    keep = jnp.stack([(r >= 0) & (r < total_rows - 1), (c >= 0) & (c < total_cols - 1)]).astype(jnp.float32)

    dual_rows = row_halo(duals.astype(jnp.bfloat16))
    dual_cols = col_halo(duals.astype(jnp.bfloat16), dual_rows)
    partial = jnp.einsum("bm,mhw->bhw", library, abundance.astype(jnp.bfloat16), preferred_element_type=jnp.float32)
    axis = "lib"
    count = lax.axis_size(axis)
    if count == 2:
        other = lax.ppermute(partial.astype(jnp.bfloat16), axis, [(0, 1), (1, 0)])
        total = partial + other.astype(jnp.float32)
    else:
        total = lax.psum(partial, axis)
    resid = (total - reflectance.astype(jnp.float32)).astype(jnp.bfloat16)
    descent = jnp.einsum("bm,bhw->mhw", library, resid, preferred_element_type=jnp.float32)
    start = abundance - 0.1 * descent
    narrow = start.astype(jnp.bfloat16)
    start_rows = row_halo(narrow)
    start_cols = col_halo(narrow, start_rows)

    block = BLOCK
    while maps % block:
        block //= 2
    one = lambda *dims: pl.BlockSpec((block,) + dims, lambda i: (i, 0, 0))
    two = lambda *dims: pl.BlockSpec((2, block) + dims, lambda i: (0, i, 0, 0))
    return pl.pallas_call(
        step_kernel,
        grid=(maps // block,),
        out_shape=(
            jax.ShapeDtypeStruct(abundance.shape, jnp.float32),
            jax.ShapeDtypeStruct(duals.shape, jnp.float32),
        ),
        in_specs=[
            one(height, width),
            two(height, width),
            one(2 * HALO, width),
            one(tall, LANES),
            two(2 * HALO, width),
            two(tall, LANES),
            pl.BlockSpec((2, tall, wide), lambda i: (0, 0, 0)),
        ],
        out_specs=(one(height, width), two(height, width)),
        compiler_params=pltpu.CompilerParams(
            dimension_semantics=("arbitrary",), vmem_limit_bytes=48 * 1024 * 1024
        ),
    )(start, duals, start_rows, start_cols, dual_rows, dual_cols, keep)


def solution(mesh):
    placed = (
        P("lib", "row", "col"),
        P(None, "lib", "row", "col"),
        P(None, "row", "col"),
        P(None, "lib"),
    )
    return jax.shard_map(
        on_device,
        mesh=mesh,
        in_specs=placed,
        out_specs=(P("lib", "row", "col"), P(None, "lib", "row", "col")),
        check_vma=False,
    )
```
